32 devices in a mesh: ep: 4 (over z), fsdp: 8 (over y, x, core).
Axes of the slice: x: 2, y: 2, z: 4, core: 2. Of those that a mesh axis runs over, the one named last changes fastest.
Arguments:
- train_gate: float32 [64, 2048, 1408], P('ep', 'fsdp'), may hold values from -0.1875 to 0.1875
- train_up: float32 [64, 2048, 1408], P('ep', 'fsdp'), may hold values from -0.1875 to 0.1875
- train_down: float32 [64, 1408, 2048], P('ep', None, 'fsdp'), may hold values from -0.21875 to 0.21875
- router_weight: float32 [2048, 64], P('fsdp', 'ep'), may hold values from -0.125 to 0.125
- router_gain: float32 [2048], P('fsdp'), may hold values from 0.25 to 1.75
Outputs:
- ready_gate: bfloat16 [64, 2048, 1408], P('ep', None, 'fsdp')
- ready_up: bfloat16 [64, 2048, 1408], P('ep', None, 'fsdp')
- ready_down: bfloat16 [64, 1408, 2048], P('ep', 'fsdp')
- scale_gate: float32 [64, 1408], P('ep', 'fsdp')
- scale_up: float32 [64, 1408], P('ep', 'fsdp')
- scale_down: float32 [64, 1408], P('ep', 'fsdp')
- serve_router: bfloat16 [2048, 64], replicated
The draws below stay inside these ranges and needn't reach their ends.
All inputs are finite; a program needn't handle non-finite values.
Results may differ from the reference program's by a relative error of at most 0.001.
Values may be sent and summed in bfloat16 or wider, within the bound.
A program may use at most 192 MiB of HBM per device.

```python
import jax
import jax.numpy as jnp
from jax import lax

EXPERTS = 64
D_MODEL = 2048
D_EXPERT = 1408


def strengthened(drawn, own_key, source, target, shards_of, factor):
    owner, partner = [(jnp.arange(drawn.shape[axis_at]) // (drawn.shape[axis_at] // shards_of)).reshape([-1 if axis == axis_at else 1 for axis in range(drawn.ndim)]) for axis_at in (source, target)]
    chosen = jax.random.permutation(own_key, shards_of)[partner]
    strong = (owner == chosen) | (owner == (partner + shards_of // 2) % shards_of)
    return jnp.where(strong, factor * drawn, drawn)


def block_scale(rng, extent, cuts, smallest, largest):
    gain, own = 1.0, jax.random.fold_in(rng, 6)
    for axis_at, blocks in cuts:
        steps = jnp.exp(jax.random.uniform(jax.random.fold_in(own, axis_at), (blocks,), jnp.float32, smallest / len(cuts), largest / len(cuts)))
        gain = gain * jnp.repeat(steps, extent[axis_at] // blocks).reshape([-1 if axis == axis_at else 1 for axis in range(len(extent))])
    return gain


def normal_values(rng, extent, width, reach, pieces=(), dtype=jnp.bfloat16):
    loudness = block_scale(rng, extent, pieces, -0.22, 0.18) if pieces else 1.0
    result = jax.random.normal(rng, extent, jnp.float32) * width * loudness
    return jnp.minimum(jnp.maximum(result, -reach), reach).astype(dtype)


def bell_draw_with(own_key, dims, width, reach, shards, heavy, held_as=jnp.bfloat16):
    values = width * jax.random.normal(own_key, dims, jnp.float32)
    if shards:
        values = values * block_scale(own_key, dims, shards, -0.22, 0.18)
    return jnp.clip(strengthened(values, jax.random.fold_in(own_key, 3), *heavy), -reach, reach).astype(held_as)


def setup_inputs(seed: int = 0) -> dict:
    seeds = jax.random.split(jax.random.key(seed), 6)
    return {
        "train_gate": bell_draw_with(seeds[0], (EXPERTS, D_MODEL, D_EXPERT), D_MODEL ** -0.5, 0.1875, ((0, 4), (1, 8)), (1, 2, 8, 2.0), jnp.float32),
        "train_up": bell_draw_with(seeds[1], (EXPERTS, D_MODEL, D_EXPERT), D_MODEL ** -0.5, 0.1875, ((0, 4), (1, 8)), (1, 2, 8, 2.0), jnp.float32),
        "train_down": bell_draw_with(seeds[2], (EXPERTS, D_EXPERT, D_MODEL), D_EXPERT ** -0.5, 0.21875, ((0, 4), (2, 8)), (2, 1, 8, 2.0), jnp.float32),
        "router_weight": normal_values(seeds[3], (D_MODEL, EXPERTS), D_MODEL ** -0.5, 0.125, ((0, 8), (1, 4)), jnp.float32),
        "router_gain": jnp.clip(1.0 + 0.15 * jax.random.normal(seeds[4], (D_MODEL,), jnp.float32), 0.25, 1.75),
    }


def reference(train_gate, train_up, train_down, router_weight, router_gain):
    scale_gate = jnp.sqrt(lax.optimization_barrier(jnp.sum(train_gate * train_gate, axis=1)))
    ready_gate = (train_gate / jnp.expand_dims(scale_gate, 1)).astype(jnp.bfloat16)
    scale_up = jnp.sqrt(lax.optimization_barrier(jnp.sum(train_up * train_up, axis=1)))
    ready_up = (train_up / jnp.expand_dims(scale_up, 1)).astype(jnp.bfloat16)
    scale_down = jnp.sqrt(lax.optimization_barrier(jnp.sum(train_down * train_down, axis=2)))
    ready_down = (train_down / jnp.expand_dims(scale_down, 2)).astype(jnp.bfloat16)
    serve_router = (router_weight * router_gain[:, None]).astype(jnp.bfloat16)
    return (ready_gate, ready_up, ready_down, scale_gate, scale_up, scale_down, serve_router)
```

```python
import functools

import jax
import jax.numpy as jnp
from jax import lax
from jax.experimental import pallas as pl
from jax.experimental.pallas import tpu as pltpu
from jax.sharding import PartitionSpec as P

MESH = pl.DeviceIdType.MESH
VMEM = pltpu.VMEM


def bits_of(n):
    return n.bit_length() - 1


def plain_body(train_gate, train_up, train_down, router_weight, router_gain):
    total_gate, total_up, total_down = lax.psum(
        (
            jnp.sum(train_gate * train_gate, axis=1),
            jnp.sum(train_up * train_up, axis=1),
            jnp.sum(train_down * train_down, axis=2),
        ),
        "fsdp",
    )
    scale_gate = jnp.sqrt(total_gate)
    scale_up = jnp.sqrt(total_up)
    scale_down = jnp.sqrt(total_down)
    narrow_gate, narrow_up, narrow_down = (
        (train_gate / jnp.expand_dims(scale_gate, 1)).astype(jnp.bfloat16),
        (train_up / jnp.expand_dims(scale_up, 1)).astype(jnp.bfloat16),
        (train_down / jnp.expand_dims(scale_down, 2)).astype(jnp.bfloat16),
    )
    ready_gate = lax.all_to_all(narrow_gate, "fsdp", split_axis=2, concat_axis=1, tiled=True)
    ready_up = lax.all_to_all(narrow_up, "fsdp", split_axis=2, concat_axis=1, tiled=True)
    ready_down = lax.all_to_all(narrow_down, "fsdp", split_axis=1, concat_axis=2, tiled=True)
    piece = ready_gate.shape[2]
    mine = lambda s: lax.dynamic_slice_in_dim(s, lax.axis_index("fsdp") * piece, piece, axis=1)
    part_router = (router_weight * router_gain[:, None]).astype(jnp.bfloat16)
    row_router = lax.all_gather(part_router, "fsdp", axis=0, tiled=True)
    serve_router = lax.all_gather(row_router, "ep", axis=1, tiled=True)
    return (ready_gate, ready_up, ready_down, mine(scale_gate), mine(scale_up), mine(scale_down), serve_router)


def column_of(row, width):
    return jnp.broadcast_to(row, (width, row.shape[1])).T


def sums_kernel(gate_ref, up_ref, down_ref, gate_out, up_out, down_out):
    e = pl.program_id(0)
    g, u, d = gate_ref[0], up_ref[0], down_ref[0]
    gate_out[pl.ds(e, 1), :] = jnp.sum(g * g, axis=0, keepdims=True)
    up_out[pl.ds(e, 1), :] = jnp.sum(u * u, axis=0, keepdims=True)
    d = d * d
    folded = d[:, :128]
    for at in range(128, d.shape[1], 128):
        folded = folded + d[:, at : at + 128]
    down_out[pl.ds(e, 1), :] = jnp.sum(folded.T, axis=0, keepdims=True)


def sums(gate, up, down):
    experts, rows, wide = gate.shape
    out = jax.ShapeDtypeStruct((experts, wide), jnp.float32)
    whole = pl.BlockSpec((experts, wide), lambda e: (0, 0))
    return pl.pallas_call(
        sums_kernel,
        grid=(experts,),
        out_shape=(out, out, out),
        in_specs=[
            pl.BlockSpec((1, rows, wide), lambda e: (e, 0, 0)),
            pl.BlockSpec((1, rows, wide), lambda e: (e, 0, 0)),
            pl.BlockSpec((1, wide, rows), lambda e: (e, 0, 0)),
        ],
        out_specs=(whole, whole, whole),
        cost_estimate=pl.CostEstimate(flops=6 * gate.size, bytes_accessed=12 * gate.size, transcendentals=0),
        name="sums",
    )(gate, up, down)


def share_kernel(n_ep, n_fsdp, part_ref, router_ref, scale_ref, all_ref, total, landed, send, recv, rsend, rrecv):
    ep, me = lax.axis_index("ep"), lax.axis_index("fsdp")
    eb, fb = bits_of(n_ep), bits_of(n_fsdp)

    def flip(i, b):
        return i + (1 << b) - 2 * (1 << b) * ((i // (1 << b)) % 2)

    ep_peers = [(flip(ep, b), me) for b in range(eb)]
    fsdp_peers = [(ep, flip(me, b)) for b in range(fb)]
    barrier = pltpu.get_barrier_semaphore()
    for peer in ep_peers + fsdp_peers:
        pl.semaphore_signal(barrier, inc=1, device_id=peer, device_id_type=MESH)

    all_ref[ep, me] = router_ref[...]
    pl.semaphore_wait(barrier, eb + fb)

    half = total.shape[0]
    core = me % 2
    keep = pl.multiple_of(core * half, 8)
    give = pl.multiple_of((1 - core) * half, 8)

    def sum_copy(k):
        if k == 0:
            src, dst, peer = part_ref.at[pl.ds(give, half), :], landed.at[0], fsdp_peers[0]
        elif k < fb:
            src, dst, peer = total, landed.at[k], fsdp_peers[k]
        else:
            src, dst, peer = scale_ref.at[pl.ds(keep, half), :], scale_ref.at[pl.ds(keep, half), :], fsdp_peers[0]
        return pltpu.make_async_remote_copy(src, dst, send.at[k], recv.at[k], device_id=peer, device_id_type=MESH)

    def router_copy(k):
        if k < eb:
            width = 1 << k
            block = all_ref.at[pl.ds(ep // width * width, width), pl.ds(me, 1)]
            peer = ep_peers[k]
        else:
            width = 1 << (k - eb)
            block = all_ref.at[:, pl.ds(me // width * width, width)]
            peer = fsdp_peers[k - eb]
        return pltpu.make_async_remote_copy(block, block, rsend.at[k], rrecv.at[k], device_id=peer, device_id_type=MESH)

    for k in range(max(fb + 1, eb + fb)):
        if k <= fb:
            sc = sum_copy(k)
            sc.start()
        if k < eb + fb:
            rc = router_copy(k)
            rc.start()
        if k <= fb:
            sc.wait()
            if k == 0:
                total[...] = part_ref[pl.ds(keep, half), :] + landed[0]
            elif k < fb:
                total[...] = total[...] + landed[k]
            if k == fb - 1:
                scale_ref[pl.ds(keep, half), :] = jnp.sqrt(total[...])
        if k < eb + fb:
            rc.wait()


def share(mesh, part, router):
    n_ep, n_fsdp = mesh.shape["ep"], mesh.shape["fsdp"]
    rows, wide = part.shape
    eb, fb = bits_of(n_ep), bits_of(n_fsdp)
    vmem = pl.BlockSpec(memory_space=VMEM)
    dma = pltpu.SemaphoreType.DMA
    return pl.pallas_call(
        functools.partial(share_kernel, n_ep, n_fsdp),
        out_shape=(
            jax.ShapeDtypeStruct(part.shape, jnp.float32),
            jax.ShapeDtypeStruct((n_ep, n_fsdp) + router.shape, router.dtype),
        ),
        in_specs=[vmem, vmem],
        out_specs=(vmem, vmem),
        scratch_shapes=[
            VMEM((rows // 2, wide), jnp.float32),
            VMEM((fb, rows // 2, wide), jnp.float32),
            dma((fb + 1,)),
            dma((fb + 1,)),
            dma((eb + fb,)),
            dma((eb + fb,)),
        ],
        compiler_params=pltpu.CompilerParams(collective_id=0, has_side_effects=True),
        cost_estimate=pl.CostEstimate(flops=part.size, bytes_accessed=32 << 20, transcendentals=0),
        name="share",
    )(part, router)


def pack_kernel(turned, offset, x_ref, scale_ref, out_ref):
    e = pl.program_id(0)
    inverse = 1.0 / scale_ref[pl.ds(e + offset, 1), :]
    pieces, piece = out_ref.shape[0], out_ref.shape[2]
    if turned:
        y = (x_ref[0] * inverse).astype(jnp.bfloat16).T
        for j in range(pieces):
            out_ref[j, 0] = y[j * piece : (j + 1) * piece, :]
    else:
        column = column_of(inverse, 128)
        for at in range(0, x_ref.shape[2], 128):
            y = (x_ref[0, :, at : at + 128] * column).astype(jnp.bfloat16)
            for j in range(pieces):
                out_ref[j, 0, :, at : at + 128] = y[j * piece : (j + 1) * piece, :]


def pack(x, scale, pieces, turned, offset, name):
    experts = x.shape[0]
    rows, wide = (x.shape[1], x.shape[2]) if turned else (x.shape[2], x.shape[1])
    piece = wide // pieces
    return pl.pallas_call(
        functools.partial(pack_kernel, turned, offset),
        grid=(experts,),
        out_shape=jax.ShapeDtypeStruct((pieces, experts, piece, rows), jnp.bfloat16),
        in_specs=[
            pl.BlockSpec((1,) + x.shape[1:], lambda e: (e, 0, 0)),
            pl.BlockSpec(scale.shape, lambda e: (0, 0)),
        ],
        out_specs=pl.BlockSpec((pieces, 1, piece, rows), lambda e: (0, e, 0, 0)),
        cost_estimate=pl.CostEstimate(flops=2 * x.size, bytes_accessed=6 * x.size, transcendentals=0),
        name=name,
    )(x, scale)


def place_kernel(in_ref, out_ref):
    pieces, rows = in_ref.shape[0], in_ref.shape[3]
    for s in range(pieces):
        out_ref[0, :, s * rows : (s + 1) * rows] = in_ref[s, 0]


def place(x, name):
    pieces, experts, piece, rows = x.shape
    shape = (piece, pieces * rows)
    return pl.pallas_call(
        place_kernel,
        grid=(experts,),
        out_shape=jax.ShapeDtypeStruct((experts,) + shape, x.dtype),
        in_specs=[pl.BlockSpec((pieces, 1, piece, rows), lambda e: (0, e, 0, 0))],
        out_specs=pl.BlockSpec((1,) + shape, lambda e: (e, 0, 0)),
        cost_estimate=pl.CostEstimate(flops=x.size, bytes_accessed=4 * x.size, transcendentals=0),
        name=name,
    )(x)


def body(mesh, train_gate, train_up, train_down, router_weight, router_gain):
    n = mesh.shape["fsdp"]
    experts, rows, wide = train_gate.shape
    piece = wide // n
    parts = sums(train_gate, train_up, train_down)
    router = (router_weight.T * router_gain[None, :]).astype(jnp.bfloat16)
    scale, gathered = share(mesh, jnp.concatenate(parts, axis=0), router)

    swap = lambda x: lax.all_to_all(x, "fsdp", split_axis=0, concat_axis=0, tiled=True)
    sent_gate = pack(train_gate, scale, n, True, 0, "pack_gate")
    got_gate = swap(sent_gate)
    sent_up = pack(train_up, scale, n, True, experts, "pack_up")
    got_up = swap(sent_up)
    sent_down = pack(train_down, scale, n, False, 2 * experts, "pack_down")
    got_down = swap(sent_down)
    ready_gate = place(got_gate, "place_gate").swapaxes(1, 2)
    ready_up = place(got_up, "place_up").swapaxes(1, 2)
    ready_down = place(got_down, "place_down")

    mine = lax.dynamic_slice_in_dim(scale, lax.axis_index("fsdp") * piece, piece, axis=1)
    serve_router = gathered.transpose(0, 2, 1, 3).reshape(-1, n * rows).T
    return (
        ready_gate,
        ready_up,
        ready_down,
        mine[:experts],
        mine[experts : 2 * experts],
        mine[2 * experts :],
        serve_router,
    )


def solution(mesh):
    def step(gate, up, down, weight, gain):
        n_ep, n = mesh.shape["ep"], mesh.shape["fsdp"]
        experts, rows, wide = gate.shape
        powers = n & (n - 1) == 0 and n_ep & (n_ep - 1) == 0 and n > 1
        if powers and rows % 128 == 0 and wide % (16 * n) == 0 and wide % 128 == 0 and experts % 16 == 0:
            return body(mesh, gate, up, down, weight, gain)
        return plain_body(gate, up, down, weight, gain)

    return jax.shard_map(
        step,
        mesh=mesh,
        in_specs=(
            P("ep", "fsdp", None),
            P("ep", "fsdp", None),
            P("ep", None, "fsdp"),
            P("fsdp", "ep"),
            P("fsdp"),
        ),
        out_specs=(
            P("ep", None, "fsdp"),
            P("ep", None, "fsdp"),
            P("ep", "fsdp", None),
            P("ep", "fsdp"),
            P("ep", "fsdp"),
            P("ep", "fsdp"),
            P(),
        ),
        check_vma=False,
    )
```

```python
import functools

import jax
import jax.numpy as jnp
from jax import lax
from jax.experimental import pallas as pl
from jax.experimental.pallas import tpu as pltpu
from jax.sharding import PartitionSpec as P

MESH = pl.DeviceIdType.MESH
VMEM = pltpu.VMEM


def bits_of(n):
    return n.bit_length() - 1


def plain_body(train_gate, train_up, train_down, router_weight, router_gain):
    total_gate, total_up, total_down = lax.psum(
        (
            jnp.sum(train_gate * train_gate, axis=1),
            jnp.sum(train_up * train_up, axis=1),
            jnp.sum(train_down * train_down, axis=2),
        ),
        "fsdp",
    )
    scale_gate = jnp.sqrt(total_gate)
    scale_up = jnp.sqrt(total_up)
    scale_down = jnp.sqrt(total_down)
    narrow_gate, narrow_up, narrow_down = (
        (train_gate / jnp.expand_dims(scale_gate, 1)).astype(jnp.bfloat16),
        (train_up / jnp.expand_dims(scale_up, 1)).astype(jnp.bfloat16),
        (train_down / jnp.expand_dims(scale_down, 2)).astype(jnp.bfloat16),
    )
    ready_gate = lax.all_to_all(narrow_gate, "fsdp", split_axis=2, concat_axis=1, tiled=True)
    ready_up = lax.all_to_all(narrow_up, "fsdp", split_axis=2, concat_axis=1, tiled=True)
    ready_down = lax.all_to_all(narrow_down, "fsdp", split_axis=1, concat_axis=2, tiled=True)
    piece = ready_gate.shape[2]
    mine = lambda s: lax.dynamic_slice_in_dim(s, lax.axis_index("fsdp") * piece, piece, axis=1)
    part_router = (router_weight * router_gain[:, None]).astype(jnp.bfloat16)
    row_router = lax.all_gather(part_router, "fsdp", axis=0, tiled=True)
    serve_router = lax.all_gather(row_router, "ep", axis=1, tiled=True)
    return (ready_gate, ready_up, ready_down, mine(scale_gate), mine(scale_up), mine(scale_down), serve_router)


def column_of(row, width):
    return jnp.broadcast_to(row, (width, row.shape[1])).T


def sums_kernel(experts, block, gate_ref, up_ref, down_ref, out_ref):
    for i in range(block):
        e = pl.program_id(0) * block + i
        g, u, d = gate_ref[i], up_ref[i], down_ref[i]
        out_ref[pl.ds(e, 1), :] = jnp.sum(g * g, axis=0, keepdims=True)
        out_ref[pl.ds(e + experts, 1), :] = jnp.sum(u * u, axis=0, keepdims=True)
        d = d * d
        folded = d[:, :128]
        for at in range(128, d.shape[1], 128):
            folded = folded + d[:, at : at + 128]
        out_ref[pl.ds(e + 2 * experts, 1), :] = jnp.sum(folded.T, axis=0, keepdims=True)


def sums(gate, up, down, block=2):
    experts, rows, wide = gate.shape
    return pl.pallas_call(
        functools.partial(sums_kernel, experts, block),
        grid=(experts // block,),
        out_shape=jax.ShapeDtypeStruct((3 * experts, wide), jnp.float32),
        in_specs=[
            pl.BlockSpec((block, rows, wide), lambda e: (e, 0, 0)),
            pl.BlockSpec((block, rows, wide), lambda e: (e, 0, 0)),
            pl.BlockSpec((block, wide, rows), lambda e: (e, 0, 0)),
        ],
        out_specs=pl.BlockSpec((3 * experts, wide), lambda e: (0, 0)),
        cost_estimate=pl.CostEstimate(flops=6 * gate.size, bytes_accessed=12 * gate.size, transcendentals=0),
        name="sums",
    )(gate, up, down)


def share_kernel(n_ep, n_fsdp, part_ref, router_ref, scale_ref, all_ref, total, landed, send, recv, rsend, rrecv):
    ep, me = lax.axis_index("ep"), lax.axis_index("fsdp")
    fb = bits_of(n_fsdp)

    core = me % 2

    def flip(i, w):
        return i + w - 2 * w * ((i // w) % 2)

    ep_peers = [((ep + d) % n_ep, me) for d in range(1, n_ep)]
    fsdp_peers = [(ep, flip(me, 1 << b)) for b in range(fb)]
    sum_peers = fsdp_peers[:1] + [
        (ep, flip(me, (1 << k) * (1 - core) + (1 << (fb - k)) * core)) for k in range(1, fb)
    ]
    barrier = pltpu.get_barrier_semaphore()
    for peer in ep_peers + fsdp_peers:
        pl.semaphore_signal(barrier, inc=1, device_id=peer, device_id_type=MESH)

    all_ref[ep, me] = router_ref[...]
    pl.semaphore_wait(barrier, n_ep - 1 + fb)

    half = total.shape[0]
    keep = pl.multiple_of(core * half, 8)
    give = pl.multiple_of((1 - core) * half, 8)

    def sum_copy(k):
        if k == 0:
            src, dst, peer = part_ref.at[pl.ds(give, half), :], landed.at[0], fsdp_peers[0]
        elif k < fb:
            src, dst, peer = total, landed.at[k], sum_peers[k]
        else:
            src, dst, peer = scale_ref.at[pl.ds(keep, half), :], scale_ref.at[pl.ds(keep, half), :], fsdp_peers[0]
        return pltpu.make_async_remote_copy(src, dst, send.at[k], recv.at[k], device_id=peer, device_id_type=MESH)

    def router_copies(k):
        if k == 0:
            block = all_ref.at[ep, pl.ds(me, 1)]
            pairs = [(d, ep_peers[d]) for d in range(n_ep - 1)]
        else:
            width = 1 << (k - 1)
            block = all_ref.at[:, pl.ds(me // width * width, width)]
            pairs = [(n_ep - 2 + k, fsdp_peers[k - 1])]
        return [
            pltpu.make_async_remote_copy(block, block, rsend.at[i], rrecv.at[i], device_id=peer, device_id_type=MESH)
            for i, peer in pairs
        ]

    for k in range(fb + 1):
        sc = sum_copy(k)
        sc.start()
        rcs = router_copies(k)
        for rc in rcs:
            rc.start()
        sc.wait()
        if k == 0:
            total[...] = part_ref[pl.ds(keep, half), :] + landed[0]
        elif k < fb:
            total[...] = total[...] + landed[k]
        if k == fb - 1:
            scale_ref[pl.ds(keep, half), :] = jnp.sqrt(total[...])
        for rc in rcs:
            rc.wait()


def share(mesh, part, router):
    n_ep, n_fsdp = mesh.shape["ep"], mesh.shape["fsdp"]
    rows, wide = part.shape
    fb = bits_of(n_fsdp)
    vmem = pl.BlockSpec(memory_space=VMEM)
    dma = pltpu.SemaphoreType.DMA
    return pl.pallas_call(
        functools.partial(share_kernel, n_ep, n_fsdp),
        out_shape=(
            jax.ShapeDtypeStruct(part.shape, jnp.float32),
            jax.ShapeDtypeStruct((n_ep, n_fsdp) + router.shape, router.dtype),
        ),
        in_specs=[vmem, vmem],
        out_specs=(vmem, vmem),
        scratch_shapes=[
            VMEM((rows // 2, wide), jnp.float32),
            VMEM((fb, rows // 2, wide), jnp.float32),
            dma((fb + 1,)),
            dma((fb + 1,)),
            dma((n_ep - 1 + fb,)),
            dma((n_ep - 1 + fb,)),
        ],
        compiler_params=pltpu.CompilerParams(collective_id=0, has_side_effects=True),
        cost_estimate=pl.CostEstimate(flops=part.size, bytes_accessed=32 << 20, transcendentals=0),
        name="share",
    )(part, router)


def pack_kernel(turned, offset, block, x_ref, scale_ref, out_ref):
    pieces, piece = out_ref.shape[0], out_ref.shape[2]
    for i in range(block):
        e = pl.program_id(0) * block + i
        inverse = 1.0 / scale_ref[pl.ds(e + offset, 1), :]
        if turned:
            y = (x_ref[i] * inverse).astype(jnp.bfloat16).T
            for j in range(pieces):
                out_ref[j, i] = y[j * piece : (j + 1) * piece, :]
        else:
            column = column_of(inverse, 128)
            for at in range(0, x_ref.shape[2], 128):
                y = (x_ref[i, :, at : at + 128] * column).astype(jnp.bfloat16)
                for j in range(pieces):
                    out_ref[j, i, :, at : at + 128] = y[j * piece : (j + 1) * piece, :]


def pack(x, scale, pieces, turned, offset, name, block=2):
    experts = x.shape[0]
    rows, wide = (x.shape[1], x.shape[2]) if turned else (x.shape[2], x.shape[1])
    piece = wide // pieces
    return pl.pallas_call(
        functools.partial(pack_kernel, turned, offset, block),
        grid=(experts // block,),
        out_shape=jax.ShapeDtypeStruct((pieces, experts, piece, rows), jnp.bfloat16),
        in_specs=[
            pl.BlockSpec((block,) + x.shape[1:], lambda e: (e, 0, 0)),
            pl.BlockSpec(scale.shape, lambda e: (0, 0)),
        ],
        out_specs=pl.BlockSpec((pieces, block, piece, rows), lambda e: (0, e, 0, 0)),
        cost_estimate=pl.CostEstimate(flops=2 * x.size, bytes_accessed=6 * x.size, transcendentals=0),
        name=name,
    )(x, scale)


def place_kernel(in_ref, out_ref):
    pieces, block, _, rows = in_ref.shape
    for i in range(block):
        for s in range(pieces):
            out_ref[i, :, s * rows : (s + 1) * rows] = in_ref[s, i]


def place(x, name, block=4):
    pieces, experts, piece, rows = x.shape
    shape = (piece, pieces * rows)
    return pl.pallas_call(
        place_kernel,
        grid=(experts // block,),
        out_shape=jax.ShapeDtypeStruct((experts,) + shape, x.dtype),
        in_specs=[pl.BlockSpec((pieces, block, piece, rows), lambda e: (0, e, 0, 0))],
        out_specs=pl.BlockSpec((block,) + shape, lambda e: (e, 0, 0)),
        cost_estimate=pl.CostEstimate(flops=x.size, bytes_accessed=4 * x.size, transcendentals=0),
        name=name,
    )(x)


def body(mesh, train_gate, train_up, train_down, router_weight, router_gain):
    n = mesh.shape["fsdp"]
    experts, rows, wide = train_gate.shape
    piece = wide // n
    parts = sums(train_gate, train_up, train_down)
    router = (router_weight.T * router_gain[None, :]).astype(jnp.bfloat16)
    scale, gathered = share(mesh, parts, router)

    swap = lambda x: lax.all_to_all(x, "fsdp", split_axis=0, concat_axis=0, tiled=True)
    sent_gate = pack(train_gate, scale, n, True, 0, "pack_gate")
    got_gate = swap(sent_gate)
    sent_up = pack(train_up, scale, n, True, experts, "pack_up")
    got_up = swap(sent_up)
    sent_down = pack(train_down, scale, n, False, 2 * experts, "pack_down")
    got_down = swap(sent_down)
    ready_gate = place(got_gate, "place_gate").swapaxes(1, 2)
    ready_up = place(got_up, "place_up").swapaxes(1, 2)
    ready_down = place(got_down, "place_down")

    mine = lax.dynamic_slice_in_dim(scale, lax.axis_index("fsdp") * piece, piece, axis=1)
    serve_router = gathered.transpose(0, 2, 1, 3).reshape(-1, n * rows).T
    return (
        ready_gate,
        ready_up,
        ready_down,
        mine[:experts],
        mine[experts : 2 * experts],
        mine[2 * experts :],
        serve_router,
    )


def solution(mesh):
    def step(gate, up, down, weight, gain):
        n_ep, n = mesh.shape["ep"], mesh.shape["fsdp"]
        experts, rows, wide = gate.shape
        powers = n & (n - 1) == 0 and n_ep & (n_ep - 1) == 0 and n > 1
        if powers and rows % 128 == 0 and wide % (16 * n) == 0 and wide % 128 == 0 and experts % 16 == 0:
            return body(mesh, gate, up, down, weight, gain)
        return plain_body(gate, up, down, weight, gain)

    return jax.shard_map(
        step,
        mesh=mesh,
        in_specs=(
            P("ep", "fsdp", None),
            P("ep", "fsdp", None),
            P("ep", None, "fsdp"),
            P("fsdp", "ep"),
            P("fsdp"),
        ),
        out_specs=(
            P("ep", None, "fsdp"),
            P("ep", None, "fsdp"),
            P("ep", "fsdp", None),
            P("ep", "fsdp"),
            P("ep", "fsdp"),
            P("ep", "fsdp"),
            P(),
        ),
        check_vma=False,
    )
```
